32 devices in a mesh: segment: 4 (over y, core), dp: 8 (over z, x).
Axes of the slice: x: 2, y: 2, z: 4, core: 2. Of those that a mesh axis runs over, the one named last changes fastest.
Arguments:
- token_ids: int32 [1024], P('dp'), may hold values from 0 to 38015, as said below
- table: bfloat16 [4752, 28672], P('segment', 'dp'), may hold values from -6 to 6
- out_grad: bfloat16 [1024, 3584], P('dp', 'segment'), may hold values from -6 to 6
Outputs:
- embedded: bfloat16 [1024, 3584], P('dp')
- table_grad: bfloat16 [4752, 28672], P('segment', 'dp')
The draws below stay inside these ranges and needn't reach their ends.
Inputs may be any that keep to these rules, and one draw needn't show every extreme that they name: `token_ids`: in the 128 tokens of each data group, at most 16 ids lie in one segment's slice of 9504 rows with one residue modulo 8; in every data group some segment and residue has exactly 16.
All inputs are finite; a program needn't handle non-finite values.
Results may differ from the reference program's by a relative error of at most 0.001.
Values may be sent and summed in bfloat16 or wider, within the bound.
A program may use at most 64 MiB of HBM per device.

```python
import jax
import jax.numpy as jnp
from jax import lax

D = 3584
ROWS_SECTION = 9504
PACK = 8
TOK_DEV = 128
VOCAB = 38016
TOKENS = 1024


def draw_token_ids(key, part):
    groups = TOKENS // TOK_DEV
    segments = VOCAB // ROWS_SECTION
    buckets = segments * PACK
    capacity = TOK_DEV // PACK
    lines = ROWS_SECTION // PACK
    global_hot = jax.random.randint(jax.random.fold_in(key, 11), (), 0, buckets)

    def one_group(group):
        group_key = jax.random.fold_in(key, 100 + group)
        keys = jax.random.split(group_key, 7)
        order = jax.random.permutation(keys[0], buckets)
        use_global = jax.random.randint(keys[1], (), 0, 2)
        hot = jnp.where(use_global == 1, global_hot, order[0])
        hot_pos = jnp.argmax(order == hot)
        order = order.at[hot_pos].set(order[0]).at[0].set(hot)
        spread = jax.random.randint(keys[2], (), 7, buckets)
        position = jnp.arange(TOK_DEV)
        bucket = jnp.where(position < capacity, order[0], order[1 + (position - capacity) % spread])
        hot_line = jax.random.randint(keys[3], (TOK_DEV,), 0, min(lines, 4))
        any_line = jax.random.randint(keys[4], (TOK_DEV,), 0, lines)
        pick = jax.random.randint(keys[5], (TOK_DEV,), 0, 2)
        line = jnp.where(pick == 1, hot_line, any_line)
        ids = bucket // PACK * ROWS_SECTION + line * PACK + bucket % PACK
        shuffle = jax.random.permutation(keys[6], TOK_DEV)
        return ids[shuffle]
    return jax.vmap(one_group)(jnp.arange(groups)).reshape(-1).astype(jnp.int32)


def shard_levels(rng, dims, cuts, least, top_value):
    level = 1.0
    for axis_at, shards_of in cuts:
        draws = jax.random.uniform(jax.random.fold_in(jax.random.fold_in(rng, 6), axis_at), (shards_of,), jnp.float32, least / len(cuts), top_value / len(cuts))
        level = level * jnp.repeat(jnp.exp(draws), dims[axis_at] // shards_of).reshape((-1,) + (1,) * (len(dims) - 1 - axis_at))
    return level


def normal_values(own_key, shape, deviation, most, cuts=(), held_as=jnp.bfloat16):
    drawn = jax.random.normal(own_key, shape, jnp.float32) * deviation
    if len(cuts) > 0:
        drawn = shard_levels(own_key, shape, cuts, -0.22, 0.18) * drawn
    return jnp.clip(drawn, min=-most, max=most).astype(held_as)


def setup_inputs(seed: int = 0) -> dict:
    splits = jax.random.split(jax.random.key(seed), 4)
    token_ids = draw_token_ids(jax.random.fold_in(splits[3], 71), 0)
    table = normal_values(splits[1], (VOCAB // PACK, PACK * D), 1.0, 6.0, ((0, 4), (1, 8)))
    out_grad = normal_values(splits[2], (TOKENS, D), 1.0, 6.0, ((0, 8), (1, 4)))
    return {"token_ids": token_ids, "table": table, "out_grad": out_grad}


def reference(token_ids, table, out_grad):
    flat = table.reshape(VOCAB, D)
    embedded = jnp.take(flat, token_ids, axis=0)
    width = 128 if D % 128 == 0 else D
    blocks = D // width
    pieces = out_grad.reshape(TOKENS, blocks, width).transpose(1, 0, 2)

    def accumulate(piece):
        total = jnp.zeros((VOCAB, width), jnp.float32).at[token_ids].add(piece.astype(jnp.float32))
        return total.astype(jnp.bfloat16)

    summed = lax.map(accumulate, pieces)
    table_grad = summed.transpose(1, 0, 2).reshape(VOCAB // PACK, PACK * D)
    return embedded, table_grad
```

```python
import functools

import jax
import jax.numpy as jnp
from jax import lax
from jax.experimental import pallas as pl
from jax.experimental.pallas import tpu as pltpu
from jax.sharding import PartitionSpec as P

PACK = 8
BF = jnp.bfloat16
F32 = jnp.float32


def flip(index, bit):
    return index + bit - 2 * bit * ((index // bit) % 2)


def push(src, dst, send, recv, peer):
    copy = pltpu.make_async_remote_copy(
        src_ref=src,
        dst_ref=dst,
        send_sem=send,
        recv_sem=recv,
        device_id=peer,
        device_id_type=pl.DeviceIdType.MESH,
    )
    copy.start()
    return copy


def select(ids, first, lines, slot, cap):
    rows, tok = ids.shape
    local = ids - first
    owned = (local >= 0) & (local < lines * PACK) & (ids % PACK == slot)
    before = lax.broadcasted_iota(jnp.int32, (tok, tok), 0) < lax.broadcasted_iota(
        jnp.int32, (tok, tok), 1
    )
    rank = jnp.dot(
        jnp.where(owned, 1.0, 0.0).astype(BF),
        jnp.where(before, 1.0, 0.0).astype(BF),
        preferred_element_type=F32,
    )
    want = lax.broadcasted_iota(jnp.int32, (rows, tok), 0) % cap
    return owned & (rank.astype(jnp.int32) == want), local


def kernel(
    groups, segs, inside, chunk,
    ids_ref, table_ref, grad_ref,
    emb_ref, back_ref, hot_ref,
    ids_all, table, rows_out, rows_in, grads, back_out, part, halves, total,
    table_sem, ids_sem, grad_sem, fwd_sem, bwd_sem, seg_sem, copy_sem,
):
    dp = lax.axis_index("dp")
    seg = lax.axis_index("segment")
    lines, width = table.shape
    cap, tok = ids_ref.shape
    quarters = groups // PACK
    chunks = width // chunk
    half = tok // 2
    first = seg * lines * PACK
    core = seg % 2
    offsets = sorted(range(1, groups), key=lambda k: -min(k, groups - k))
    bits = [1 << b for b in range(segs.bit_length() - 1)]

    load = pltpu.make_async_copy(table_ref, table, table_sem)
    load.start()
    barrier = pltpu.get_barrier_semaphore()
    for k in offsets:
        pl.semaphore_signal(
            barrier, inc=1, device_id={"dp": (dp + k) % groups},
            device_id_type=pl.DeviceIdType.MESH,
        )
    for b in bits:
        pl.semaphore_signal(
            barrier, inc=1, device_id={"segment": flip(seg, b)},
            device_id_type=pl.DeviceIdType.MESH,
        )
    pl.semaphore_wait(barrier, len(offsets) + len(bits))

    sent = []
    ids_copies = []
    for k in offsets:
        ids_copies.append(push(
            ids_ref, ids_all.at[dp], ids_sem.at[0, k], ids_sem.at[1, k],
            {"dp": (dp + k) % groups},
        ))
    ids_all[dp] = ids_ref[...]

    grad_waits = []
    if inside:
        grads[seg] = grad_ref[...]
        held = [seg]
        stage = 0
        pending = []
        far = bits[::-1]
        copies = [push(
            grad_ref, grads.at[seg], grad_sem.at[0, 0], grad_sem.at[1, 0],
            {"segment": flip(seg, far[0])},
        )]
        stage = 1
        grad_waits = copies

    mine = jnp.concatenate([ids_ref[...]] * PACK, axis=0)
    slot_of = lax.broadcasted_iota(jnp.int32, (PACK * cap, tok), 0) // cap
    pick, _ = select(mine, first, lines, slot_of, cap)
    pick = jnp.where(pick, 1.0, 0.0)
    spread = pick.T.astype(BF)
    pick = pick.astype(BF)

    for copy in ids_copies:
        copy.wait_recv()
    named, local = select(
        ids_all[...].reshape(groups * cap, tok), first, lines, dp // quarters, cap
    )
    line = jnp.sum(
        jnp.where(named, (local // PACK + 1).astype(F32), 0.0), axis=1, keepdims=True
    ).astype(jnp.int32) - 1
    hot = jnp.where(
        lax.broadcasted_iota(jnp.int32, (groups * cap, lines), 1) == line, 1.0, 0.0
    ).astype(BF)
    hot_ref[...] = hot

    load.wait()
    fwd = []
    for f in range(chunks):
        cols = pl.ds(f * chunk, chunk)
        got = jnp.dot(hot_ref[...], table[:, cols], preferred_element_type=F32).astype(BF)
        rows_out[:, :, cols] = got.reshape(groups, cap, chunk)
        for k in offsets:
            peer = (dp + k) % groups
            fwd.append(push(
                rows_out.at[peer, :, cols], rows_in.at[dp, :, cols],
                fwd_sem.at[0, k, f], fwd_sem.at[1, k, f], {"dp": peer},
            ))
    rows_in[dp] = rows_out[dp]

    if inside:
        held = [seg]
        slot = 0
        for level, b in enumerate(far):
            if level > 0:
                copies = []
                for piece in held:
                    slot += 1
                    copies.append(push(
                        grads.at[piece], grads.at[piece],
                        grad_sem.at[0, slot], grad_sem.at[1, slot], {"segment": flip(seg, b)},
                    ))
            for copy in copies:
                copy.wait_recv()
            sent += copies
            held = held + [flip(piece, b) for piece in held]
        piece_width = grads.shape[2]
    else:
        piece_width = width

    whole = quarters * width
    for f in range(whole // piece_width):
        q, off = (f * piece_width) // width, (f * piece_width) % width
        if inside:
            block = grads[f]
        else:
            block = grad_ref[:, f * piece_width:(f + 1) * piece_width]
        got = jnp.dot(pick, block, preferred_element_type=F32).astype(BF)
        for r in range(PACK):
            back_out[r * quarters + q, :, off:off + piece_width] = got[r * cap:(r + 1) * cap]
    bwd = []
    for k in offsets:
        peer = (dp + k) % groups
        bwd.append(push(
            back_out.at[peer], back_ref.at[dp], bwd_sem.at[0, k], bwd_sem.at[1, k], {"dp": peer},
        ))
    back_ref[dp] = back_out[dp]

    for copy in fwd:
        copy.wait_recv()
    for q in range(quarters):
        for f in range(chunks):
            got = jnp.concatenate(
                [rows_in[r * quarters + q, :, f * chunk:(f + 1) * chunk] for r in range(PACK)], axis=0
            )
            got = jnp.dot(spread, got, preferred_element_type=F32).astype(BF)
            at = q * width + f * chunk
            part[:, :, at:at + chunk] = got.reshape(2, half, chunk)

    copy = push(
        part.at[1 - core], halves.at[0], seg_sem.at[0, 0], seg_sem.at[1, 0],
        {"segment": flip(seg, 1)},
    )
    copy.wait_recv()
    sent.append(copy)
    total[0] = part[core] + halves[0]
    for n, b in enumerate(bits[1:]):
        copy = push(
            total.at[n], halves.at[n + 1], seg_sem.at[0, n + 1], seg_sem.at[1, n + 1],
            {"segment": flip(seg, b)},
        )
        copy.wait_recv()
        sent.append(copy)
        total[n + 1] = total[n] + halves[n + 1]
    last = len(bits) - 1
    copy = push(
        total.at[last], emb_ref.at[core], seg_sem.at[0, last + 1], seg_sem.at[1, last + 1],
        {"segment": flip(seg, 1)},
    )
    emb_ref[core] = total[last]
    copy.wait_recv()
    sent.append(copy)

    for copy in bwd:
        copy.wait_recv()
    for copy in sent + ids_copies + fwd + bwd:
        copy.wait_send()


def body(token_ids, table, out_grad, groups, segs):
    lines, width = table.shape
    tok, piece = out_grad.shape
    depth = segs * piece
    cap = tok // PACK
    inside = piece % 128 == 0 and width % piece == 0
    if not inside:
        out_grad = lax.all_gather(out_grad, "segment", axis=1, tiled=True)
    chunk = width // 4 if width % 512 == 0 else width
    chunks = width // chunk
    levels = segs.bit_length() - 1
    vmem = pl.BlockSpec(memory_space=pltpu.VMEM)
    dma = pltpu.SemaphoreType.DMA
    emb, back, hot = pl.pallas_call(
        functools.partial(kernel, groups, segs, inside, chunk),
        out_shape=(
            jax.ShapeDtypeStruct((2, tok // 2, depth), BF),
            jax.ShapeDtypeStruct((groups, cap, width), BF),
            jax.ShapeDtypeStruct((groups * cap, lines), BF),
        ),
        in_specs=[vmem, pl.BlockSpec(memory_space=pl.ANY), vmem],
        out_specs=(vmem, vmem, vmem),
        scratch_shapes=[
            pltpu.VMEM((groups, cap, tok), jnp.int32),
            pltpu.VMEM((lines, width), BF),
            pltpu.VMEM((groups, cap, width), BF),
            pltpu.VMEM((groups, cap, width), BF),
            pltpu.VMEM((segs, tok, piece) if inside else (1, 16, 128), BF),
            pltpu.VMEM((groups, cap, width), BF),
            pltpu.VMEM((2, tok // 2, depth), BF),
            pltpu.VMEM((levels, tok // 2, depth), BF),
            pltpu.VMEM((levels, tok // 2, depth), BF),
            dma,
            dma((2, groups)),
            dma((2, segs)),
            dma((2, groups, chunks)),
            dma((2, groups)),
            dma((2, levels + 1)),
            dma,
        ],
        compiler_params=pltpu.CompilerParams(
            collective_id=0, has_side_effects=True, vmem_limit_bytes=48 << 20
        ),
    )(jnp.broadcast_to(token_ids[None, :], (cap, tok)), table, out_grad)
    grad = lax.dot_general(
        hot, back.reshape(groups * cap, width), (((0,), (0,)), ((), ())),
        preferred_element_type=F32,
    )
    return emb.reshape(tok, depth), grad.astype(BF)


def solution(mesh):
    placed = (P("dp"), P("segment", "dp"), P("dp", "segment"))
    return jax.shard_map(
        functools.partial(body, groups=mesh.shape["dp"], segs=mesh.shape["segment"]),
        mesh=mesh,
        in_specs=placed,
        out_specs=(P("dp", None), P("segment", "dp")),
        check_vma=False,
    )
```

```python
import functools

import jax
import jax.numpy as jnp
from jax import lax
from jax.experimental import pallas as pl
from jax.experimental.pallas import tpu as pltpu
from jax.sharding import PartitionSpec as P

PACK = 8
BF = jnp.bfloat16
F32 = jnp.float32


def flip(index, bit):
    return index + bit - 2 * bit * ((index // bit) % 2)


def push(src, dst, send, recv, peer):
    copy = pltpu.make_async_remote_copy(
        src_ref=src,
        dst_ref=dst,
        send_sem=send,
        recv_sem=recv,
        device_id=peer,
        device_id_type=pl.DeviceIdType.MESH,
    )
    copy.start()
    return copy


def select(ids, first, lines, slot, cap):
    rows, tok = ids.shape
    local = ids - first
    owned = (local >= 0) & (local < lines * PACK) & (ids % PACK == slot)
    before = lax.broadcasted_iota(jnp.int32, (tok, tok), 0) < lax.broadcasted_iota(
        jnp.int32, (tok, tok), 1
    )
    rank = jnp.dot(
        jnp.where(owned, 1.0, 0.0).astype(BF),
        jnp.where(before, 1.0, 0.0).astype(BF),
        preferred_element_type=F32,
    )
    want = lax.broadcasted_iota(jnp.int32, (rows, tok), 0) % cap
    return owned & (rank.astype(jnp.int32) == want), local


def kernel(
    groups, segs, inside, chunk,
    ids_ref, table_ref, grad_ref,
    emb_ref, back_ref, hot_ref,
    ids_mine, ids_all, table, rows_out, rows_in, grads, back_out, part, halves, total,
    load_sem, ids_sem, raw_sem, grad_sem, fwd_sem, bwd_sem, seg_sem,
):
    dp = lax.axis_index("dp")
    seg = lax.axis_index("segment")
    lines, width = table.shape
    cap, tok = ids_mine.shape
    quarters = groups // PACK
    chunks = width // chunk
    half = tok // 2
    near = groups // 2
    base = (dp // near) * near
    mirror = (dp + near) % groups
    first = seg * lines * PACK
    core = seg % 2
    offsets = sorted(range(1, groups), key=lambda k: -min(k, groups - k))
    bits = [1 << b for b in range(segs.bit_length() - 1)]
    far = bits[::-1] if inside else []
    own = seg if inside else 0

    load_grad = pltpu.make_async_copy(grad_ref, grads.at[0, own], load_sem.at[0])
    load_grad.start()
    load = pltpu.make_async_copy(table_ref, table, load_sem.at[1])
    load.start()
    ids_mine[...] = jnp.broadcast_to(ids_ref[...], (cap, tok))
    barrier = pltpu.get_barrier_semaphore()
    for k in offsets:
        pl.semaphore_signal(
            barrier, inc=1, device_id={"dp": (dp + k) % groups},
            device_id_type=pl.DeviceIdType.MESH,
        )
    for b in bits:
        pl.semaphore_signal(
            barrier, inc=1, device_id={"segment": flip(seg, b)},
            device_id_type=pl.DeviceIdType.MESH,
        )
    load_grad.wait()
    pl.semaphore_wait(barrier, len(offsets) + len(bits))

    sent = []
    ids_copies = []
    for k in offsets:
        ids_copies.append(push(
            ids_mine, ids_all.at[dp], ids_sem.at[0, k], ids_sem.at[1, k],
            {"dp": (dp + k) % groups},
        ))
    raw = push(
        grads.at[0, own], grads.at[1, own], raw_sem.at[0], raw_sem.at[1], {"dp": mirror}
    )

    held = [[own], [own]]
    flying = [[], []]

    def gather_start(kind, level):
        for piece in held[kind]:
            n = len(sent_of[kind])
            copy = push(
                grads.at[kind, piece], grads.at[kind, piece],
                grad_sem.at[0, kind, n], grad_sem.at[1, kind, n],
                {"segment": flip(seg, far[level])},
            )
            sent_of[kind].append(copy)
            flying[kind].append(copy)

    def gather_wait(kind, level):
        for copy in flying[kind]:
            copy.wait_recv()
        flying[kind] = []
        held[kind] = held[kind] + [flip(piece, far[level]) for piece in held[kind]]

    sent_of = [[], []]
    if far:
        gather_start(0, 0)
    ids_all[dp] = ids_mine[...]

    slot_of = lax.broadcasted_iota(jnp.int32, (PACK * cap, tok), 0) // cap
    pick, _ = select(
        jnp.concatenate([ids_mine[...]] * PACK, axis=0), first, lines, slot_of, cap
    )
    scatter = jnp.where(pick, 1.0, 0.0).T.astype(BF)

    for copy in ids_copies:
        copy.wait_recv()
    named, local = select(
        ids_all[...].reshape(groups * cap, tok), first, lines, dp // quarters, cap
    )
    line = jnp.sum(
        jnp.where(named, (local // PACK + 1).astype(F32), 0.0), axis=1, keepdims=True
    ).astype(jnp.int32) - 1
    hot = jnp.where(
        lax.broadcasted_iota(jnp.int32, (groups * cap, lines), 1) == line, 1.0, 0.0
    ).astype(BF)
    hot_ref[...] = hot

    load.wait()
    fwd = []
    for f in range(chunks):
        cols = pl.ds(f * chunk, chunk)
        got = jnp.dot(hot_ref[...], table[:, cols], preferred_element_type=F32).astype(BF)
        rows_out[:, :, cols] = got.reshape(groups, cap, chunk)
        fwd.append([])
        for k in offsets:
            peer = (dp + k) % groups
            fwd[f].append(push(
                rows_out.at[peer, :, cols], rows_in.at[dp, :, cols],
                fwd_sem.at[0, k, f], fwd_sem.at[1, k, f], {"dp": peer},
            ))
    rows_in[dp] = rows_out[dp]

    slots_near = PACK // 2
    near_slot = base // quarters + lax.broadcasted_iota(
        jnp.int32, (slots_near * cap, tok), 0
    ) // cap
    depth = quarters * width
    piece_width = grads.shape[3]
    step = min(piece_width, width)
    bwd = []

    def dispatch(kind, group):
        pick, _ = select(
            jnp.concatenate([ids_all[group]] * slots_near, axis=0), first, lines, near_slot, cap
        )
        pick = jnp.where(pick, 1.0, 0.0).astype(BF)
        for at in range(0, depth, step):
            q, off = at // width, at % width
            inner = at % piece_width
            got = jnp.dot(
                pick, grads[kind, at // piece_width, :, inner:inner + step],
                preferred_element_type=F32,
            ).astype(BF)
            for r in range(slots_near):
                back_out[kind, r * quarters + q, :, off:off + step] = got[r * cap:(r + 1) * cap]
        for k in range(1, near):
            to = (dp - base + k) % near
            bwd.append(push(
                back_out.at[kind, to], back_ref.at[group],
                bwd_sem.at[0, kind, k], bwd_sem.at[1, kind, k], {"dp": base + to},
            ))
        back_ref[group] = back_out[kind, dp - base]

    for level in range(len(far)):
        if level > 0:
            gather_start(0, level)
        gather_wait(0, level)
    dispatch(0, dp)
    raw.wait_recv()
    for level in range(len(far)):
        gather_start(1, level)
        gather_wait(1, level)
    dispatch(1, mirror)

    tiles = [(f, q) for f in range(chunks) for q in range(quarters)]
    stages = len(bits) + 2
    moving = {}

    def seg_push(src, dst, level, n, bit):
        copy = push(
            src, dst, seg_sem.at[0, level, n], seg_sem.at[1, level, n],
            {"segment": flip(seg, bit)},
        )
        sent.append(copy)
        moving[n] = copy

    def advance(n, stage):
        f, q = tiles[n]
        at = q * width + f * chunk
        cols = pl.ds(at, chunk)
        if stage == 0:
            if q == 0:
                for copy in fwd[f]:
                    copy.wait_recv()
            got = jnp.concatenate(
                [rows_in[r * quarters + q, :, f * chunk:(f + 1) * chunk] for r in range(PACK)], axis=0
            )
            got = jnp.dot(scatter, got, preferred_element_type=F32).astype(BF)
            part[:, :, cols] = got.reshape(2, half, chunk)
            seg_push(part.at[1 - core, :, cols], halves.at[0, :, cols], 0, n, 1)
            return
        moving[n].wait_recv()
        if stage == stages - 1:
            return
        if stage == 1:
            total[0, :, cols] = part[core, :, cols] + halves[0, :, cols]
        else:
            total[stage - 1, :, cols] = total[stage - 2, :, cols] + halves[stage - 1, :, cols]
        src = total.at[stage - 1, :, cols]
        if stage < len(bits):
            seg_push(src, halves.at[stage, :, cols], stage, n, bits[stage])
        else:
            seg_push(src, emb_ref.at[core, :, cols], stage, n, 1)
            emb_ref[core, :, cols] = total[stage - 1, :, cols]

    for wave in range(len(tiles) + stages - 1):
        for stage in range(stages):
            if 0 <= wave - stage < len(tiles):
                advance(wave - stage, stage)

    for copy in bwd:
        copy.wait_recv()
    for copies in [sent, ids_copies, [raw], bwd] + sent_of + fwd:
        for copy in copies:
            copy.wait_send()


def body(token_ids, table, out_grad, groups, segs):
    lines, width = table.shape
    tok, piece = out_grad.shape
    depth = segs * piece
    cap = tok // PACK
    inside = piece % 128 == 0 and width % piece == 0
    if not inside:
        out_grad = lax.all_gather(out_grad, "segment", axis=1, tiled=True)
    pieces = segs if inside else 1
    chunk = width // 4 if width % 512 == 0 else width
    chunks = width // chunk
    levels = segs.bit_length() - 1
    vmem = pl.BlockSpec(memory_space=pltpu.VMEM)
    hbm = pl.BlockSpec(memory_space=pltpu.HBM)
    dma = pltpu.SemaphoreType.DMA
    emb, back, hot = pl.pallas_call(
        functools.partial(kernel, groups, segs, inside, chunk),
        out_shape=(
            jax.ShapeDtypeStruct((2, tok // 2, depth), BF),
            jax.ShapeDtypeStruct((groups, cap, width), BF),
            jax.ShapeDtypeStruct((groups * cap, lines), BF),
        ),
        in_specs=[vmem, hbm, hbm],
        out_specs=(vmem, vmem, vmem),
        scratch_shapes=[
            pltpu.VMEM((cap, tok), jnp.int32),
            pltpu.VMEM((groups, cap, tok), jnp.int32),
            pltpu.VMEM((lines, width), BF),
            pltpu.VMEM((groups, cap, width), BF),
            pltpu.VMEM((groups, cap, width), BF),
            pltpu.VMEM((2, pieces, tok, depth // pieces), BF),
            pltpu.VMEM((2, groups // 2, cap, width), BF),
            pltpu.VMEM((2, tok // 2, depth), BF),
            pltpu.VMEM((levels, tok // 2, depth), BF),
            pltpu.VMEM((levels, tok // 2, depth), BF),
            dma((2,)),
            dma((2, groups)),
            dma((2,)),
            dma((2, 2, segs)),
            dma((2, groups, chunks)),
            dma((2, 2, groups // 2)),
            dma((2, levels + 1, chunks * (groups // PACK))),
        ],
        compiler_params=pltpu.CompilerParams(
            collective_id=0, has_side_effects=True, vmem_limit_bytes=48 << 20
        ),
    )(token_ids[None, :], table, out_grad)
    grad = lax.dot_general(
        hot, back.reshape(groups * cap, width), (((0,), (0,)), ((), ())),
        preferred_element_type=F32,
    )
    return emb.reshape(tok, depth), grad.astype(BF)


def solution(mesh):
    placed = (P("dp"), P("segment", "dp"), P("dp", "segment"))
    return jax.shard_map(
        functools.partial(body, groups=mesh.shape["dp"], segs=mesh.shape["segment"]),
        mesh=mesh,
        in_specs=placed,
        out_specs=(P("dp", None), P("segment", "dp")),
        check_vma=False,
    )
```

```python
import functools

import jax
import jax.numpy as jnp
from jax import lax
from jax.experimental import pallas as pl
from jax.experimental.pallas import tpu as pltpu
from jax.sharding import PartitionSpec as P

PACK = 8
BF = jnp.bfloat16
F32 = jnp.float32


def flip(index, bit):
    return index + bit - 2 * bit * ((index // bit) % 2)


def push(src, dst, send, recv, peer):
    copy = pltpu.make_async_remote_copy(
        src_ref=src,
        dst_ref=dst,
        send_sem=send,
        recv_sem=recv,
        device_id=peer,
        device_id_type=pl.DeviceIdType.MESH,
    )
    copy.start()
    return copy


def select(ids, first, lines, slot, cap):
    rows, tok = ids.shape
    local = ids - first
    owned = (local >= 0) & (local < lines * PACK) & (ids % PACK == slot)
    before = lax.broadcasted_iota(jnp.int32, (tok, tok), 0) < lax.broadcasted_iota(
        jnp.int32, (tok, tok), 1
    )
    rank = jnp.dot(
        jnp.where(owned, 1.0, 0.0).astype(BF),
        jnp.where(before, 1.0, 0.0).astype(BF),
        preferred_element_type=F32,
    )
    want = lax.broadcasted_iota(jnp.int32, (rows, tok), 0) % cap
    return owned & (rank.astype(jnp.int32) == want), local


def kernel(
    groups, segs, inside, chunk,
    ids_ref, table_ref, grad_ref,
    emb_ref, back_ref, hot_ref,
    ids_mine, ids_all, table, rows_out, rows_in, grads, back_out, part, halves, total,
    load_sem, ids_sem, raw_sem, grad_sem, fwd_sem, bwd_sem, seg_sem,
):
    dp = lax.axis_index("dp")
    seg = lax.axis_index("segment")
    lines, width = table.shape
    cap, tok = ids_mine.shape
    quarters = groups // PACK
    chunks = width // chunk
    half = tok // 2
    near = groups // 2
    base = (dp // near) * near
    mirror = (dp + near) % groups
    first = seg * lines * PACK
    core = seg % 2
    offsets = sorted(range(1, groups), key=lambda k: -min(k, groups - k))
    bits = [1 << b for b in range(segs.bit_length() - 1)]
    far = bits[::-1] if inside else []
    own = seg if inside else 0

    load_grad = pltpu.make_async_copy(grad_ref, grads.at[0, own], load_sem.at[0])
    load_grad.start()
    load = pltpu.make_async_copy(table_ref, table, load_sem.at[1])
    load.start()
    ids_mine[...] = jnp.broadcast_to(ids_ref[...], (cap, tok))
    barrier = pltpu.get_barrier_semaphore()
    for k in offsets:
        pl.semaphore_signal(
            barrier, inc=1, device_id={"dp": (dp + k) % groups},
            device_id_type=pl.DeviceIdType.MESH,
        )
    for b in bits:
        pl.semaphore_signal(
            barrier, inc=1, device_id={"segment": flip(seg, b)},
            device_id_type=pl.DeviceIdType.MESH,
        )
    load_grad.wait()
    pl.semaphore_wait(barrier, len(offsets) + len(bits))

    sent = []
    ids_copies = []
    for k in offsets:
        ids_copies.append(push(
            ids_mine, ids_all.at[dp], ids_sem.at[0, k], ids_sem.at[1, k],
            {"dp": (dp + k) % groups},
        ))

    raw = push(
        grads.at[0, own], grads.at[1, own], raw_sem.at[0], raw_sem.at[1], {"dp": mirror}
    )

    held = [[own], [own]]
    flying = [[], []]

    def gather_start(kind, level):
        for piece in held[kind]:
            n = len(sent_of[kind])
            copy = push(
                grads.at[kind, piece], grads.at[kind, piece],
                grad_sem.at[0, kind, n], grad_sem.at[1, kind, n],
                {"segment": flip(seg, far[level])},
            )
            sent_of[kind].append(copy)
            flying[kind].append(copy)

    def gather_wait(kind, level):
        for copy in flying[kind]:
            copy.wait_recv()
        flying[kind] = []
        held[kind] = held[kind] + [flip(piece, far[level]) for piece in held[kind]]

    sent_of = [[], []]
    ids_all[dp] = ids_mine[...]

    slot_of = lax.broadcasted_iota(jnp.int32, (PACK * cap, tok), 0) // cap
    pick, _ = select(
        jnp.concatenate([ids_mine[...]] * PACK, axis=0), first, lines, slot_of, cap
    )
    scatter = jnp.where(pick, 1.0, 0.0).T.astype(BF)

    for copy in ids_copies:
        copy.wait_recv()
    if far:
        gather_start(0, 0)
    named, local = select(
        ids_all[...].reshape(groups * cap, tok), first, lines, dp // quarters, cap
    )
    line = jnp.sum(
        jnp.where(named, (local // PACK + 1).astype(F32), 0.0), axis=1, keepdims=True
    ).astype(jnp.int32) - 1
    hot = jnp.where(
        lax.broadcasted_iota(jnp.int32, (groups * cap, lines), 1) == line, 1.0, 0.0
    ).astype(BF)
    hot_ref[...] = hot

    def fetch(f, n, peer):
        cols = pl.ds(f * chunk, chunk)
        fwd[f].append(push(
            rows_out.at[peer, :, cols], rows_in.at[dp, :, cols],
            fwd_sem.at[0, n, f], fwd_sem.at[1, n, f], {"dp": peer},
        ))

    load.wait()
    fwd = []
    for f in range(chunks):
        cols = pl.ds(f * chunk, chunk)
        got = jnp.dot(hot_ref[...], table[:, cols], preferred_element_type=F32).astype(BF)
        rows_out[:, :, cols] = got.reshape(groups, cap, chunk)
        fwd.append([])
        for k in range(1, near):
            fetch(f, k, base + (dp - base + k) % near)
    for f in range(chunks):
        for k in range(near):
            fetch(f, near + k, (near - base) + (dp - base + k) % near)
    rows_in[dp] = rows_out[dp]

    slots_near = PACK // 2
    near_slot = base // quarters + lax.broadcasted_iota(
        jnp.int32, (slots_near * cap, tok), 0
    ) // cap
    depth = quarters * width
    piece_width = grads.shape[3]
    step = min(piece_width, width)
    bwd = []

    def dispatch(kind, group):
        pick, _ = select(
            jnp.concatenate([ids_all[group]] * slots_near, axis=0), first, lines, near_slot, cap
        )
        pick = jnp.where(pick, 1.0, 0.0).astype(BF)
        for at in range(0, depth, step):
            q, off = at // width, at % width
            inner = at % piece_width
            got = jnp.dot(
                pick, grads[kind, at // piece_width, :, inner:inner + step],
                preferred_element_type=F32,
            ).astype(BF)
            for r in range(slots_near):
                back_out[kind, r * quarters + q, :, off:off + step] = got[r * cap:(r + 1) * cap]
        for k in range(1, near):
            to = (dp - base + k) % near
            bwd.append(push(
                back_out.at[kind, to], back_ref.at[group],
                bwd_sem.at[0, kind, k], bwd_sem.at[1, kind, k], {"dp": base + to},
            ))
        back_ref[group] = back_out[kind, dp - base]

    for level in range(len(far)):
        if level > 0:
            gather_start(0, level)
        gather_wait(0, level)
    dispatch(0, dp)
    tiles = [(f, q) for f in range(chunks) for q in range(quarters)]
    stages = len(bits) + 2
    moving = {}

    def seg_push(src, dst, level, n, bit):
        copy = push(
            src, dst, seg_sem.at[0, level, n], seg_sem.at[1, level, n],
            {"segment": flip(seg, bit)},
        )
        sent.append(copy)
        moving[n] = copy

    def advance(n, stage):
        f, q = tiles[n]
        at = q * width + f * chunk
        cols = pl.ds(at, chunk)
        if stage == 0:
            if q == 0:
                for copy in fwd[f]:
                    copy.wait_recv()
            got = jnp.concatenate(
                [rows_in[r * quarters + q, :, f * chunk:(f + 1) * chunk] for r in range(PACK)], axis=0
            )
            got = jnp.dot(scatter, got, preferred_element_type=F32).astype(BF)
            part[:, :, cols] = got.reshape(2, half, chunk)
            seg_push(part.at[1 - core, :, cols], halves.at[0, :, cols], 0, n, 1)
            return
        moving[n].wait_recv()
        if stage == stages - 1:
            return
        if stage == 1:
            total[0, :, cols] = part[core, :, cols] + halves[0, :, cols]
        else:
            total[stage - 1, :, cols] = total[stage - 2, :, cols] + halves[stage - 1, :, cols]
        src = total.at[stage - 1, :, cols]
        if stage < len(bits):
            seg_push(src, halves.at[stage, :, cols], stage, n, bits[stage])
        else:
            seg_push(src, emb_ref.at[core, :, cols], stage, n, 1)
            emb_ref[core, :, cols] = total[stage - 1, :, cols]

    for wave in range(len(tiles) + stages - 1):
        if wave == 0:
            raw.wait_recv()
            if far:
                gather_start(1, 0)
            for level in range(len(far)):
                gather_wait(1, level)
                if level + 1 < len(far):
                    gather_start(1, level + 1)
            dispatch(1, mirror)
        for stage in range(stages):
            if 0 <= wave - stage < len(tiles):
                advance(wave - stage, stage)

    for copy in bwd:
        copy.wait_recv()
    for copies in [sent, ids_copies, [raw], bwd] + sent_of + fwd:
        for copy in copies:
            copy.wait_send()


def body(token_ids, table, out_grad, groups, segs):
    lines, width = table.shape
    tok, piece = out_grad.shape
    depth = segs * piece
    cap = tok // PACK
    inside = piece % 128 == 0 and width % piece == 0
    if not inside:
        out_grad = lax.all_gather(out_grad, "segment", axis=1, tiled=True)
    pieces = segs if inside else 1
    chunk = width // 4 if width % 512 == 0 else width
    chunks = width // chunk
    levels = segs.bit_length() - 1
    vmem = pl.BlockSpec(memory_space=pltpu.VMEM)
    hbm = pl.BlockSpec(memory_space=pltpu.HBM)
    dma = pltpu.SemaphoreType.DMA
    emb, back, hot = pl.pallas_call(
        functools.partial(kernel, groups, segs, inside, chunk),
        out_shape=(
            jax.ShapeDtypeStruct((2, tok // 2, depth), BF),
            jax.ShapeDtypeStruct((groups, cap, width), BF),
            jax.ShapeDtypeStruct((groups * cap, lines), BF),
        ),
        in_specs=[vmem, hbm, hbm],
        out_specs=(vmem, vmem, vmem),
        scratch_shapes=[
            pltpu.VMEM((cap, tok), jnp.int32),
            pltpu.VMEM((groups, cap, tok), jnp.int32),
            pltpu.VMEM((lines, width), BF),
            pltpu.VMEM((groups, cap, width), BF),
            pltpu.VMEM((groups, cap, width), BF),
            pltpu.VMEM((2, pieces, tok, depth // pieces), BF),
            pltpu.VMEM((2, groups // 2, cap, width), BF),
            pltpu.VMEM((2, tok // 2, depth), BF),
            pltpu.VMEM((levels, tok // 2, depth), BF),
            pltpu.VMEM((levels, tok // 2, depth), BF),
            dma((2,)),
            dma((2, groups)),
            dma((2,)),
            dma((2, 2, segs)),
            dma((2, groups, chunks)),
            dma((2, 2, groups // 2)),
            dma((2, levels + 1, chunks * (groups // PACK))),
        ],
        compiler_params=pltpu.CompilerParams(
            collective_id=0, has_side_effects=True, vmem_limit_bytes=48 << 20
        ),
    )(token_ids[None, :], table, out_grad)
    grad = lax.dot_general(
        hot, back.reshape(groups * cap, width), (((0,), (0,)), ((), ())),
        preferred_element_type=F32,
    )
    return emb.reshape(tok, depth), grad.astype(BF)


def solution(mesh):
    placed = (P("dp"), P("segment", "dp"), P("dp", "segment"))
    return jax.shard_map(
        functools.partial(body, groups=mesh.shape["dp"], segs=mesh.shape["segment"]),
        mesh=mesh,
        in_specs=placed,
        out_specs=(P("dp", None), P("segment", "dp")),
        check_vma=False,
    )
```
